16 devices in a mesh: dp: 2 (over y, z), tp: 8 (over x, core).
Axes of the slice: x: 4, y: 2, z: 1, core: 2. Of those that a mesh axis runs over, the one named last changes fastest.
The devices are a block of a 4x4x8 slice.
Arguments:
- x: bfloat16 [512, 4096], P('dp'), parts along dimension 0
- lengths: int32 [512], P('dp'), parts along dimension 0
- k_cache: bfloat16 [2, 512, 128, 8, 128], P(None, 'dp', None, 'tp'), parts along dimension 1
- v_cache: bfloat16 [2, 512, 128, 8, 128], P(None, 'dp', None, 'tp'), parts along dimension 1
- attn_norm: float32 [2, 4096], replicated
- mlp_norm: float32 [2, 4096], replicated
- w_q: bfloat16 [2, 4096, 4096], P(None, None, 'tp')
- w_k: bfloat16 [2, 4096, 1024], P(None, None, 'tp')
- w_v: bfloat16 [2, 4096, 1024], P(None, None, 'tp')
- w_o: bfloat16 [2, 4096, 4096], P(None, 'tp')
- w_gate: bfloat16 [2, 4096, 14336], P(None, None, 'tp')
- w_up: bfloat16 [2, 4096, 14336], P(None, None, 'tp')
- w_down: bfloat16 [2, 14336, 4096], P(None, 'tp')
Outputs:
- output: bfloat16 [512, 4096], P('dp'), parts along dimension 0
There are 2 independent parts. The reference program is written for one: setup_inputs(seed, part) draws one part's arguments, and reference() takes and returns one part's arrays. A program takes and returns all parts, laid end to end along the dimension named above; an argument that names none is the same for every part.
All inputs are finite; a program needn't handle non-finite values.
Results may differ from the reference program's by a relative error of at most 0.02.
Values are sent between devices in bfloat16 or wider.
A program may use at most 768 MiB of HBM per device.

```python
import jax
import jax.numpy as jnp
from jax import lax

D = 4096
HEADS = 32
KV_HEADS = 8
HEAD = 128
FF = 14336
BATCH = 256
SEQ = 128
TP = 8
LAYERS = 2
NORM_EPS = 1e-5
ROPE_BASE = 10000.0
Q_GAIN = 2.5
OUT_GAIN = 1.5


def draw_normal(rng_key, arr_shape, factor):
    return (jax.random.normal(rng_key, arr_shape, jnp.float32) * factor).astype(jnp.bfloat16)


def setup_inputs(seed: int = 0, part: int = 0) -> dict:
    shared_keys = jax.random.split(jax.random.key(seed), 9)
    part_keys = jax.random.split(jax.random.fold_in(jax.random.key(seed + 1), part), 4)
    width_q = HEADS * HEAD
    width_kv = KV_HEADS * HEAD
    cache_shape = (LAYERS, BATCH, SEQ, KV_HEADS, HEAD)
    lengths = jax.random.randint(part_keys[3], (BATCH,), 1, SEQ, dtype=jnp.int32)
    lengths = lengths.at[0].set(SEQ - 1).at[BATCH - 1].set(1)
    return {
        "x": draw_normal(part_keys[0], (BATCH, D), 1.0),
        "lengths": lengths,
        "k_cache": draw_normal(part_keys[1], cache_shape, 1.0),
        "v_cache": draw_normal(part_keys[2], cache_shape, 1.0),
        "attn_norm": jax.random.uniform(shared_keys[0], (LAYERS, D), jnp.float32, 0.5, 1.5),
        "mlp_norm": jax.random.uniform(shared_keys[1], (LAYERS, D), jnp.float32, 0.5, 1.5),
        "w_q": draw_normal(shared_keys[2], (LAYERS, D, width_q), Q_GAIN * D ** -0.5),
        "w_k": draw_normal(shared_keys[3], (LAYERS, D, width_kv), D ** -0.5),
        "w_v": draw_normal(shared_keys[4], (LAYERS, D, width_kv), D ** -0.5),
        "w_o": draw_normal(shared_keys[5], (LAYERS, width_q, D), OUT_GAIN * width_q ** -0.5),
        "w_gate": draw_normal(shared_keys[6], (LAYERS, D, FF), D ** -0.5),
        "w_up": draw_normal(shared_keys[7], (LAYERS, D, FF), D ** -0.5),
        "w_down": draw_normal(shared_keys[8], (LAYERS, FF, D), OUT_GAIN * FF ** -0.5),
    }


def rms_norm(hidden_in, norm_gain):
    mean_sq = jnp.mean(hidden_in * hidden_in, axis=-1, keepdims=True)
    return (hidden_in * lax.rsqrt(mean_sq + NORM_EPS) * norm_gain).astype(jnp.bfloat16)


def rope_tables(lengths):
    inv_freq = ROPE_BASE ** (-jnp.arange(0, HEAD, 2).astype(jnp.float32) / HEAD)
    angles = lengths.astype(jnp.float32)[:, None] * inv_freq[None, :]
    return jnp.cos(angles)[:, None, :], jnp.sin(angles)[:, None, :]


def apply_rope(proj_out, cos_t, sin_t):
    half_dim = proj_out.shape[-1] // 2
    first_half = proj_out[..., :half_dim]
    second_half = proj_out[..., half_dim:]
    return jnp.concatenate([first_half * cos_t - second_half * sin_t, second_half * cos_t + first_half * sin_t], axis=-1)


def attention(q_heads, k_new, v_new, k_layer, v_layer, lengths):
    batch_n = k_layer.shape[0]
    seq_n = k_layer.shape[1]
    group_n = HEADS // KV_HEADS
    inv_scale = HEAD ** -0.5
    q_group = q_heads.reshape(batch_n, KV_HEADS, group_n, HEAD).astype(jnp.float32)
    logits = jnp.einsum("bkgd,bskd->bkgs", q_group, k_layer.astype(jnp.float32)) * inv_scale
    valid_mask = jnp.arange(seq_n)[None, None, None, :] < lengths[:, None, None, None]
    logits = jnp.where(valid_mask, logits, -1e30)
    logit_new = jnp.einsum("bkgd,bkd->bkg", q_group, k_new.astype(jnp.float32)) * inv_scale
    row_max = jnp.maximum(jnp.max(logits, axis=-1), logit_new)
    prob_cache = jnp.exp(logits - row_max[..., None])
    prob_new = jnp.exp(logit_new - row_max)
    prob_sum = jnp.sum(prob_cache, axis=-1) + prob_new
    weighted = jnp.einsum("bkgs,bskd->bkgd", prob_cache.astype(jnp.bfloat16).astype(jnp.float32), v_layer.astype(jnp.float32))
    weighted = weighted + prob_new.astype(jnp.bfloat16).astype(jnp.float32)[..., None] * v_new.astype(jnp.float32)[:, :, None, :]
    return (weighted / prob_sum[..., None]).astype(jnp.bfloat16).reshape(batch_n, HEADS * HEAD)


def block_sum(activations, weight):
    act_blocks = activations.reshape(activations.shape[0], TP, -1).astype(jnp.float32)
    weight_blocks = weight.reshape(TP, -1, weight.shape[1]).astype(jnp.float32)
    partials = jnp.einsum("btk,tkn->tbn", act_blocks, weight_blocks).astype(jnp.bfloat16)
    return jnp.sum(partials.astype(jnp.float32), axis=0)


def reference(x, lengths, k_cache, v_cache, attn_norm, mlp_norm, w_q, w_k, w_v, w_o, w_gate, w_up, w_down):
    batch_n = x.shape[0]
    cos_t, sin_t = rope_tables(lengths)
    residual = x
    for layer_idx in range(LAYERS):
        resid_f = residual.astype(jnp.float32)
        normed = rms_norm(resid_f, attn_norm[layer_idx])
        q_proj = jnp.dot(normed, w_q[layer_idx], preferred_element_type=jnp.float32)
        k_proj = jnp.dot(normed, w_k[layer_idx], preferred_element_type=jnp.float32)
        q_heads = apply_rope(q_proj.reshape(batch_n, HEADS, HEAD), cos_t, sin_t).astype(jnp.bfloat16)
        k_new = apply_rope(k_proj.reshape(batch_n, KV_HEADS, HEAD), cos_t, sin_t).astype(jnp.bfloat16)
        v_new = jnp.dot(normed, w_v[layer_idx], preferred_element_type=jnp.float32).astype(jnp.bfloat16).reshape(batch_n, KV_HEADS, HEAD)
        attn_out = attention(q_heads, k_new, v_new, k_cache[layer_idx], v_cache[layer_idx], lengths)
        hidden_f = (resid_f + block_sum(attn_out, w_o[layer_idx])).astype(jnp.bfloat16).astype(jnp.float32)
        normed_mlp = rms_norm(hidden_f, mlp_norm[layer_idx])
        gate_proj = jnp.dot(normed_mlp, w_gate[layer_idx], preferred_element_type=jnp.float32)
        up_proj = jnp.dot(normed_mlp, w_up[layer_idx], preferred_element_type=jnp.float32)
        mlp_act = (jax.nn.silu(gate_proj) * up_proj).astype(jnp.bfloat16)
        residual = (hidden_f + block_sum(mlp_act, w_down[layer_idx])).astype(jnp.bfloat16)
    return residual
```

```python
import functools

import jax
import jax.numpy as jnp
from jax import lax
from jax.experimental import pallas as pl
from jax.experimental.pallas import tpu as pltpu
from jax.sharding import PartitionSpec as P

NORM_EPS = 1e-5
ROPE_BASE = 10000.0
BF = jnp.bfloat16
F32 = jnp.float32
CHUNKS = 2
TOK = 16
NKV = 4
GRP = 4
TILE = 256
COPIES = ("part", "far", "near", "relay", "ssq", "g_fwd", "g_bwd", "g_far", "p_own", "p_bwd", "p_fwd", "p_far")


def dot(a, b):
    return jnp.dot(a, b, preferred_element_type=F32)


def kernel(
    x, cos, sin, nrow, kc, vc, an, mn, wq, wk, wv, wo, wg, wu, wd, out,
    wa, wb, kbuf, vbuf, cbuf, pbuf, dbuf, xs, ys, zs, xr, yr, zr, qsum, rsum, hres, act, qs, kx, vx, osc, obf,
    sem_a, sem_b, sem_k, sem_v, sem_x, ssem, rsem,
):
    n_layers = wq.shape[0]
    batch, width = x.shape
    chunk = batch // CHUNKS
    half = width // 2
    head = kc.shape[3]
    heads = wq.shape[2] // head
    n_ff = wg.shape[2] // TILE
    n_o = wo.shape[1] // TILE
    n_q = wq.shape[2] // TILE
    n_tp = lax.axis_size("tp")
    chips = n_tp // 2
    rows = chunk // chips
    steps = chunk // TOK
    scale = head ** -0.5

    me = lax.axis_index("tp")
    core = lax.rem(me, 2)
    chip = lax.div(me, 2)
    sign = 1 - 2 * core
    fwd_chip = lax.rem(chip + sign + chips, chips)
    bwd_chip = lax.rem(chip - sign + chips, chips)
    far_chip = lax.rem(chip + 2, chips)
    fwd, bwd = fwd_chip * 2 + core, bwd_chip * 2 + core
    peer = chip * 2 + 1 - core

    def rows_of(c):
        return pl.ds(pl.multiple_of(c * rows, rows), rows)

    own_cols = pl.ds(pl.multiple_of(core * half, half), half)
    peer_cols = pl.ds(pl.multiple_of((1 - core) * half, half), half)

    def load_a(layer, t):
        src = (wg, wu)[t % 2]
        return [pltpu.make_async_copy(src.at[layer, :, pl.ds((t // 2) * TILE, TILE)], wa.at[t], sem_a.at[t])]

    def load_q(layer, t):
        return [pltpu.make_async_copy(wq.at[layer, :, pl.ds(t * TILE, TILE)], wa.at[t], sem_a.at[t])]

    def load_kv(layer):
        t = n_q
        return [
            pltpu.make_async_copy(wk.at[layer], wa.at[t, :, pl.ds(0, head)], sem_a.at[t]),
            pltpu.make_async_copy(wv.at[layer], wa.at[t, :, pl.ds(head, head)], sem_k.at[NKV]),
        ]

    def load_o(layer, t):
        return [pltpu.make_async_copy(wo.at[layer, pl.ds(t * TILE, TILE), :], wb.at[t], sem_b.at[t])]

    def load_d(layer, t):
        return [pltpu.make_async_copy(wd.at[layer, pl.ds(t * TILE, TILE), :], wb.at[t], sem_b.at[t])]

    def begin(copies, priority=1):
        for c in copies:
            c.start(priority=priority)

    def finish(copies):
        for c in copies:
            c.wait()

    def load_cache(g):
        layer = g // (CHUNKS * steps)
        tok = pl.multiple_of(lax.rem(g, CHUNKS * steps) * TOK, TOK)
        slot = lax.rem(g, NKV)
        return [
            pltpu.make_async_copy(kc.at[layer, pl.ds(tok, TOK)], kbuf.at[slot], sem_k.at[slot]),
            pltpu.make_async_copy(vc.at[layer, pl.ds(tok, TOK)], vbuf.at[slot], sem_v.at[slot]),
        ]

    def load_x(ch):
        return [
            pltpu.make_async_copy(x.at[pl.ds(ch * chunk, chunk), :], pbuf.at[ch], sem_x.at[ch, 0]),
            pltpu.make_async_copy(
                x.at[pl.ds(pl.multiple_of(ch * chunk + chip * rows, rows), rows), own_cols], hres.at[ch], sem_x.at[ch, 1]
            ),
        ]

    n_attn = n_q + 1

    begin(load_x(0), 0)
    for t in range(n_q):
        begin(load_q(0, t), 0)
    begin(load_kv(0), 0)
    for g in range(NKV):
        begin(load_cache(jnp.int32(g)), 0)
    begin(load_x(1), 0)
    for t in range(n_o):
        begin(load_o(0, t))
    for t in range(n_attn, 2 * n_ff):
        begin(load_a(0, t))
    for t in range(n_o, n_ff):
        begin(load_d(0, t))

    barrier = pltpu.get_barrier_semaphore()
    for other in (peer, fwd, bwd):
        pl.semaphore_signal(barrier, inc=1, device_id={"tp": other}, device_id_type=pl.DeviceIdType.MESH)
    pl.semaphore_wait(barrier, 3)

    def first_norm(ch):
        finish(load_x(ch))

        def body(i, _):
            r = pl.ds(pl.multiple_of(i * 16, 16), 16)
            h = pbuf[ch, r, :].astype(F32)
            inv = lax.rsqrt(jnp.mean(h * h, axis=-1, keepdims=True) + NORM_EPS)
            cbuf[ch, r, :] = (h * inv * an[0:1, :]).astype(BF)
            return 0

        lax.fori_loop(0, chunk // 16, body, 0)

    def remote(ch, name, src, dst, target):
        i = COPIES.index(name)
        return pltpu.make_async_remote_copy(
            src_ref=src,
            dst_ref=dst,
            send_sem=ssem.at[ch, i],
            recv_sem=rsem.at[ch, i],
            device_id={"tp": target},
            device_id_type=pl.DeviceIdType.MESH,
        )

    def block(ch, c, cols):
        return cbuf.at[ch, rows_of(c), cols]

    def copies_of(ch):
        d = {
            "part": remote(ch, "part", pbuf.at[ch, :, peer_cols], dbuf.at[ch], peer),
            "far": remote(ch, "far", xs.at[ch], xr.at[ch], fwd),
            "near": remote(ch, "near", ys.at[ch], yr.at[ch], bwd),
            "relay": remote(ch, "relay", zs.at[ch], zr.at[ch], fwd),
            "ssq": remote(ch, "ssq", qsum.at[ch], rsum.at[ch], peer),
        }
        for name, c, target in (
            ("g_fwd", chip, fwd), ("g_bwd", chip, bwd), ("g_far", bwd_chip, fwd),
            ("p_own", chip, peer), ("p_bwd", bwd_chip, peer), ("p_fwd", fwd_chip, peer), ("p_far", far_chip, peer),
        ):
            d[name] = remote(ch, name, block(ch, c, own_cols), block(ch, c, own_cols), target)
        return d

    def pair(ch, c):
        return pbuf[ch, rows_of(c), own_cols].astype(F32) + dbuf[ch, rows_of(c), :].astype(F32)

    def exchange(ch, gain, last):
        d = copies_of(ch)
        d["part"].wait_recv()
        xs[ch] = pair(ch, far_chip)
        d["far"].start()
        ys[ch] = pair(ch, bwd_chip)
        d["near"].start()
        yield
        d["far"].wait_recv()
        zs[ch] = xr[ch] + pair(ch, fwd_chip)
        d["relay"].start()
        yield
        d["near"].wait_recv()
        d["relay"].wait_recv()
        h = (hres[ch].astype(F32) + (pair(ch, chip) + yr[ch] + zr[ch])).astype(BF)
        if last:
            cbuf[ch, rows_of(chip), own_cols] = h
        else:
            hres[ch] = h
            hf = h.astype(F32)
            qsum[ch] = jnp.broadcast_to(jnp.sum(hf * hf, axis=-1, keepdims=True), (rows, 128))
            d["ssq"].start()
            yield
            d["ssq"].wait_recv()
            total = (qsum[ch] + rsum[ch])[:, 0:1]
            inv = lax.rsqrt(total * (1.0 / width) + NORM_EPS)
            cbuf[ch, rows_of(chip), own_cols] = (hres[ch].astype(F32) * inv * gain[:, own_cols]).astype(BF)
        for name in ("g_fwd", "g_bwd", "p_own"):
            d[name].start()
        yield
        d["g_fwd"].wait_recv()
        d["g_far"].start()
        d["p_bwd"].start()
        d["g_bwd"].wait_recv()
        d["p_fwd"].start()
        yield
        d["g_far"].wait_recv()
        d["p_far"].start()
        yield
        for name in ("p_own", "p_bwd", "p_fwd", "p_far"):
            d[name].wait_recv()
        for name in COPIES:
            if not (last and name == "ssq"):
                d[name].wait_send()

    n_col = 512
    per_half = half // n_col

    def partial_cols(ch, product, lo, hi):
        def body(n, _):
            col = lax.rem((1 - core) * half + n * n_col, width)
            cols = pl.ds(pl.multiple_of(col, n_col), n_col)
            pbuf[ch, :, cols] = product(cols).astype(BF)
            return 0

        lax.fori_loop(lo, hi, body, 0)

    def attention(layer, ch):
        tok = pl.ds(ch * chunk, chunk)
        ct, st = cos[tok, :], sin[tok, :]

        def rope(v):
            return (v * ct + pltpu.roll(v, head // 2, 1) * st).astype(BF).astype(F32)

        for t in range(n_q):
            if ch == 0:
                finish(load_q(layer, t))
            q2 = dot(cbuf[ch], wa[t])
            for i in range(TILE // head):
                h = t * (TILE // head) + i
                qs[pl.ds(h, chunk, stride=heads), :] = rope(q2[:, i * head:(i + 1) * head])
        if ch == 0:
            finish(load_kv(layer))
        kv = dot(cbuf[ch], wa[n_q])
        k_new = rope(kv[:, :head])
        v_new = kv[:, head:].astype(BF).astype(F32)
        for h in range(heads):
            kx[pl.ds(h, chunk, stride=heads), :] = k_new
            vx[pl.ds(h, chunk, stride=heads), :] = v_new
        if ch == CHUNKS - 1:
            for t in range(n_attn):
                begin(load_a(layer, t))
        yield

        def step(i, _):
            g = (layer * CHUNKS + ch) * steps + i
            slot = lax.rem(g, NKV)
            finish(load_cache(g))
            qrows = GRP * heads
            row_tok = lax.broadcasted_iota(jnp.int32, (qrows, head), 0) // heads
            pos = lax.broadcasted_iota(jnp.int32, (qrows, head), 1)
            for j in range(TOK // GRP):
                r = pl.ds(pl.multiple_of((i * (TOK // GRP) + j) * qrows, qrows), qrows)
                rn = pl.ds(pl.multiple_of(ch * chunk * heads + (i * (TOK // GRP) + j) * qrows, qrows), qrows)
                q = qs[r, :]
                kg = kbuf[slot, pl.ds(j * GRP, GRP)].reshape(GRP * kbuf.shape[2], head)
                vg = vbuf[slot, pl.ds(j * GRP, GRP)].reshape(GRP * kbuf.shape[2], head)
                lg = lax.dot_general(q.astype(BF), kg, (((1,), (1,)), ((), ())), preferred_element_type=F32) * scale
                n = nrow[rn, :]
                parts = [
                    jnp.where(pos < jnp.where(row_tok == b, n, 0), lg[:, b * head:(b + 1) * head], -1e30)
                    for b in range(GRP)
                ]
                l_new = jnp.sum(q * kx[r, :], axis=-1, keepdims=True) * scale
                top = functools.reduce(jnp.maximum, parts)
                m = jnp.maximum(jnp.max(top, axis=-1, keepdims=True), l_new)
                ps = [jnp.exp(b - m) for b in parts]
                p_new = jnp.exp(l_new - m)
                total = jnp.sum(functools.reduce(jnp.add, ps), axis=-1, keepdims=True) + p_new
                o = dot(jnp.concatenate(ps, axis=1).astype(BF), vg)
                o = o + p_new.astype(BF).astype(F32) * vx[r, :]
                osc[r, :] = o / total

            @pl.when(g + NKV < n_layers * CHUNKS * steps)
            def _():
                begin(load_cache(g + NKV), 0)

            return 0

        for lo, hi in ((0, steps // 2), (steps // 2, steps)):
            lax.fori_loop(lo, hi, step, 0)
            yield

        for h in range(heads):
            obf[:, h * head:(h + 1) * head] = osc[pl.ds(h, chunk, stride=heads), :].astype(BF)
        if ch == 0:
            for t in range(n_o):
                finish(load_o(layer, t))

        def product(cols):
            return functools.reduce(
                jnp.add, [dot(obf[:, t * TILE:(t + 1) * TILE], wb[t, :, cols]) for t in range(n_o)]
            )

        partial_cols(ch, product, 0, per_half)
        copies_of(ch)["part"].start()
        yield
        partial_cols(ch, product, per_half, 2 * per_half)
        if ch == CHUNKS - 1:
            for t in range(n_o):
                begin(load_d(layer, t))

    def mlp(layer, ch):
        more = ch == CHUNKS - 1 and layer + 1 < n_layers

        for j in range(n_ff):
            if ch == 0:
                finish(load_a(layer, 2 * j))
                finish(load_a(layer, 2 * j + 1))
            gate = dot(cbuf[ch], wa[2 * j])
            up = dot(cbuf[ch], wa[2 * j + 1])
            act[j] = (gate * (1.0 / (1.0 + jnp.exp(-gate))) * up).astype(BF)
            if more:
                for t in (2 * j, 2 * j + 1):
                    if t < n_q:
                        begin(load_q(layer + 1, t))
                    elif t == n_q:
                        begin(load_kv(layer + 1))
                    else:
                        begin(load_a(layer + 1, t))
            yield
        if ch == 0:
            for t in range(n_ff):
                finish(load_d(layer, t))

        def product(cols):
            return functools.reduce(jnp.add, [dot(act[t], wb[t, :, cols]) for t in range(n_ff)])

        partial_cols(ch, product, 0, per_half)
        copies_of(ch)["part"].start()
        yield
        partial_cols(ch, product, per_half, 2 * per_half)
        if more:
            for t in range(n_ff):
                begin(load_o(layer + 1, t) if t < n_o else load_d(layer + 1, t))

    def drain(gen):
        if gen is not None:
            for _ in gen:
                pass

    stages = [(kind, layer, ch) for layer in range(n_layers) for kind in ("attn", "mlp") for ch in range(CHUNKS)]
    pending = {}
    for kind, layer, ch in stages:
        other = pending.get(1 - ch)
        drain(pending.pop(ch, None))
        if kind == "attn" and layer == 0:
            first_norm(ch)
        for _ in (attention if kind == "attn" else mlp)(layer, ch):
            if other is not None:
                next(other, None)
        last = kind == "mlp" and layer + 1 == n_layers
        nxt = min(layer + 1, n_layers - 1)
        gain = mn.at[layer:layer + 1] if kind == "attn" else an.at[nxt:nxt + 1]
        pending[ch] = exchange(ch, gain, last)
        next(pending[ch])
    outs = []
    for ch in range(CHUNKS):
        drain(pending.pop(ch))
        outs.append(pltpu.make_async_copy(cbuf.at[ch], out.at[pl.ds(ch * chunk, chunk), :], sem_x.at[ch, 0]))
        outs[-1].start()
    for c in outs:
        c.wait()


def solution(mesh):
    cache_spec = P(None, "dp", None, "tp", None)
    col_spec = P(None, None, "tp")
    row_spec = P(None, "tp", None)
    in_specs = (P("dp", None), P("dp"), cache_spec, cache_spec, P(), P(), col_spec, col_spec, col_spec, row_spec, col_spec, col_spec, row_spec)

    def local_layers(x, lengths, k_cache, v_cache, attn_norm, mlp_norm, w_q, w_k, w_v, w_o, w_gate, w_up, w_down):
        batch, width = x.shape
        layers, _, seq, _, head = k_cache.shape
        heads = w_q.shape[2] // head
        inner = w_o.shape[1]
        ff = w_gate.shape[2]
        chips = mesh.shape["tp"] // 2
        chunk = batch // CHUNKS
        rows = chunk // chips
        half = width // 2

        inv_freq = ROPE_BASE ** (-jnp.arange(0, head, 2).astype(F32) / head)
        angles = lengths.astype(F32)[:, None] * inv_freq[None, :]
        ct, st = jnp.cos(angles), jnp.sin(angles)
        cos = jnp.concatenate([ct, ct], axis=1)
        sin = jnp.concatenate([-st, st], axis=1)
        nrow = jnp.broadcast_to(lengths[:, None, None], (batch, heads, head)).reshape(batch * heads, head)

        vmem = pl.BlockSpec(memory_space=pltpu.VMEM)
        hbm = pl.BlockSpec(memory_space=pl.ANY)
        n_wa = 2 * (ff // TILE)
        n_wb = ff // TILE
        f32_half = pltpu.VMEM((CHUNKS, rows, half), F32)
        return pl.pallas_call(
            kernel,
            out_shape=jax.ShapeDtypeStruct((batch, width), BF),
            in_specs=[hbm, vmem, vmem, vmem, hbm, hbm, vmem, vmem] + [hbm] * 7,
            out_specs=hbm,
            scratch_shapes=[
                pltpu.VMEM((n_wa, width, TILE), BF),
                pltpu.VMEM((n_wb, TILE, width), BF),
                pltpu.VMEM((NKV, TOK, seq, head), BF),
                pltpu.VMEM((NKV, TOK, seq, head), BF),
                pltpu.VMEM((CHUNKS, chunk, width), BF),
                pltpu.VMEM((CHUNKS, chunk, width), BF),
                pltpu.VMEM((CHUNKS, chunk, half), BF),
                f32_half, f32_half, f32_half, f32_half, f32_half, f32_half,
                pltpu.VMEM((CHUNKS, rows, 128), F32),
                pltpu.VMEM((CHUNKS, rows, 128), F32),
                pltpu.VMEM((CHUNKS, rows, half), BF),
                pltpu.VMEM((n_wb, chunk, TILE), BF),
                pltpu.VMEM((chunk * heads, head), F32),
                pltpu.VMEM((chunk * heads, head), F32),
                pltpu.VMEM((chunk * heads, head), F32),
                pltpu.VMEM((chunk * heads, head), F32),
                pltpu.VMEM((chunk, inner), BF),
                pltpu.SemaphoreType.DMA((n_wa,)),
                pltpu.SemaphoreType.DMA((n_wb,)),
                pltpu.SemaphoreType.DMA((NKV + 1,)),
                pltpu.SemaphoreType.DMA((NKV,)),
                pltpu.SemaphoreType.DMA((CHUNKS, 2)),
                pltpu.SemaphoreType.DMA((CHUNKS, len(COPIES))),
                pltpu.SemaphoreType.DMA((CHUNKS, len(COPIES))),
            ],
            compiler_params=pltpu.CompilerParams(
                collective_id=0, has_side_effects=True, vmem_limit_bytes=67043328
            ),
            name="decoder",
        )(
            x, cos, sin, nrow,
            k_cache.reshape(layers, batch, seq, head), v_cache.reshape(layers, batch, seq, head),
            attn_norm, mlp_norm, w_q, w_k, w_v, w_o, w_gate, w_up, w_down,
        )

    return jax.shard_map(local_layers, mesh=mesh, in_specs=in_specs, out_specs=P("dp", None), check_vma=False)
```

```python
import functools

import jax
import jax.numpy as jnp
from jax import lax
from jax.experimental import pallas as pl
from jax.experimental.pallas import tpu as pltpu
from jax.sharding import PartitionSpec as P

NORM_EPS = 1e-5
ROPE_BASE = 10000.0
BF = jnp.bfloat16
F32 = jnp.float32
CHUNKS = 2
TOK = 16
NKV = 4
GRP = 4
TILE = 256
NP = 4
LAG = 2
ONCE = ("near", "g_fwd", "g_bwd", "g_far", "p_own", "p_bwd", "p_fwd", "p_far")
COPIES = ONCE + tuple(f"{k}{p}" for k in ("part", "far", "relay") for p in range(NP))


def dot(a, b):
    return jnp.dot(a, b, preferred_element_type=F32)


def kernel(
    x, cos, sin, nrow, kc, vc, an, mn, wq, wk, wv, wo, wg, wu, wd, out,
    wa, wb, kbuf, vbuf, cbuf, pbuf, dbuf, xs, ys, zs, xr, yr, zr, hres, act, qs, kx, vx, osc, obf,
    sem_a, sem_b, sem_k, sem_v, sem_x, ssem, rsem,
):
    n_layers = wq.shape[0]
    width = x.shape[-1]
    n_tp = lax.axis_size("tp")
    chunk = n_tp * x.shape[3]
    head = kc.shape[3]
    heads = wq.shape[2] // head
    n_ff = wg.shape[2] // TILE
    n_o = wo.shape[1] // TILE
    n_q = wq.shape[2] // TILE
    chips = n_tp // 2
    rows = chunk // n_tp
    piece = width // NP
    steps = chunk // TOK
    scale = head ** -0.5

    me = lax.axis_index("tp")
    core = lax.rem(me, 2)
    chip = lax.div(me, 2)
    sign = 1 - 2 * core
    fwd_chip = lax.rem(chip + sign + chips, chips)
    bwd_chip = lax.rem(chip - sign + chips, chips)
    far_chip = lax.rem(chip + 2, chips)
    fwd, bwd = fwd_chip * 2 + core, bwd_chip * 2 + core
    peer = chip * 2 + 1 - core

    def load_a(layer, t):
        src = (wg, wu)[t % 2]
        return [pltpu.make_async_copy(src.at[layer, :, pl.ds((t // 2) * TILE, TILE)], wa.at[t], sem_a.at[t])]

    def load_q(layer, t):
        return [pltpu.make_async_copy(wq.at[layer, :, pl.ds(t * TILE, TILE)], wa.at[t], sem_a.at[t])]

    def load_kv(layer):
        t = n_q
        return [
            pltpu.make_async_copy(wk.at[layer], wa.at[t, :, pl.ds(0, head)], sem_a.at[t]),
            pltpu.make_async_copy(wv.at[layer], wa.at[t, :, pl.ds(head, head)], sem_k.at[NKV]),
        ]

    def load_o(layer, t):
        return [pltpu.make_async_copy(wo.at[layer, pl.ds(t * TILE, TILE), :], wb.at[t], sem_b.at[t])]

    def load_d(layer, t):
        return [pltpu.make_async_copy(wd.at[layer, pl.ds(t * TILE, TILE), :], wb.at[t], sem_b.at[t])]

    def begin(copies, priority=1):
        for c in copies:
            c.start(priority=priority)

    def finish(copies):
        for c in copies:
            c.wait()

    def load_cache(g):
        layer = g // (CHUNKS * steps)
        tok = pl.multiple_of(lax.rem(g, CHUNKS * steps) * TOK, TOK)
        slot = lax.rem(g, NKV)
        return [
            pltpu.make_async_copy(kc.at[layer, pl.ds(tok, TOK)], kbuf.at[slot], sem_k.at[slot]),
            pltpu.make_async_copy(vc.at[layer, pl.ds(tok, TOK)], vbuf.at[slot], sem_v.at[slot]),
        ]

    def load_x(ch):
        return [
            pltpu.make_async_copy(x.at[ch], pbuf.at[ch], sem_x.at[ch, 0]),
            pltpu.make_async_copy(x.at[ch, chip, core], hres.at[ch], sem_x.at[ch, 1]),
        ]

    n_attn = n_q + 1

    begin(load_x(0), 0)
    for t in range(n_q):
        begin(load_q(0, t), 0)
    begin(load_kv(0), 0)
    for g in range(NKV):
        begin(load_cache(jnp.int32(g)), 0)
    begin(load_x(1), 0)
    for t in range(n_o):
        begin(load_o(0, t))
    for t in range(n_attn, 2 * n_ff):
        begin(load_a(0, t))
    for t in range(n_o, n_ff):
        begin(load_d(0, t))

    barrier = pltpu.get_barrier_semaphore()
    for other in (peer, fwd, bwd):
        pl.semaphore_signal(barrier, inc=1, device_id={"tp": other}, device_id_type=pl.DeviceIdType.MESH)
    pl.semaphore_wait(barrier, 3)

    def first_norm(ch):
        finish(load_x(ch))

        def body(i, _):
            c, k = i // 2, lax.rem(i, 2)
            h = pbuf[ch, c, k].astype(F32)
            inv = lax.rsqrt(jnp.mean(h * h, axis=-1, keepdims=True) + NORM_EPS)
            cbuf[ch, c, k] = (h * inv * an[0:1, :]).astype(BF)
            return 0

        lax.fori_loop(0, n_tp, body, 0)

    def cols_of(p):
        return pl.ds(p * piece, piece)

    def remote(ch, name, src, dst, target):
        i = COPIES.index(name)
        return pltpu.make_async_remote_copy(
            src_ref=src,
            dst_ref=dst,
            send_sem=ssem.at[ch, i],
            recv_sem=rsem.at[ch, i],
            device_id={"tp": target},
            device_id_type=pl.DeviceIdType.MESH,
        )

    def copy(ch, name):
        if name in ONCE:
            if name == "near":
                return remote(ch, name, ys.at[ch], yr.at[ch], bwd)
            c, target = {
                "g_fwd": (chip, fwd), "g_bwd": (chip, bwd), "g_far": (bwd_chip, fwd),
                "p_own": (chip, peer), "p_bwd": (bwd_chip, peer), "p_fwd": (fwd_chip, peer), "p_far": (far_chip, peer),
            }[name]
            return remote(ch, name, cbuf.at[ch, c, core], cbuf.at[ch, c, core], target)
        p = int(name[-1])
        if name.startswith("part"):
            return remote(ch, name, pbuf.at[ch, :, 1 - core, :, cols_of(p)], dbuf.at[ch, :, :, cols_of(p)], peer)
        if name.startswith("far"):
            return remote(ch, name, xs.at[ch, :, cols_of(p)], xr.at[ch, :, cols_of(p)], fwd)
        return remote(ch, name, zs.at[ch, :, cols_of(p)], zr.at[ch, :, cols_of(p)], fwd)

    def pair(ch, c, cols):
        return pbuf[ch, c, core, :, cols].astype(F32) + dbuf[ch, c, :, cols].astype(F32)

    def exchange(ch, gain, last):
        for p in range(NP):
            copy(ch, f"part{p}").wait_recv()
            xs[ch, :, cols_of(p)] = pair(ch, far_chip, cols_of(p))
            copy(ch, f"far{p}").start()
            yield f"x{p}"
        ys[ch] = pair(ch, bwd_chip, slice(None))
        copy(ch, "near").start()
        yield "near"
        for p in range(NP):
            copy(ch, f"far{p}").wait_recv()
            zs[ch, :, cols_of(p)] = xr[ch, :, cols_of(p)] + pair(ch, fwd_chip, cols_of(p))
            copy(ch, f"relay{p}").start()
            yield f"z{p}"
        copy(ch, "near").wait_recv()
        for p in range(NP):
            copy(ch, f"relay{p}").wait_recv()
        h = (hres[ch].astype(F32) + (pair(ch, chip, slice(None)) + yr[ch] + zr[ch])).astype(BF)
        if last:
            cbuf[ch, chip, core] = h
        else:
            hres[ch] = h
            hf = h.astype(F32)
            inv = lax.rsqrt(jnp.mean(hf * hf, axis=-1, keepdims=True) + NORM_EPS)
            cbuf[ch, chip, core] = (hf * inv * gain[...]).astype(BF)
        for name in ("g_fwd", "g_bwd", "p_own"):
            copy(ch, name).start()
        yield "norm"
        copy(ch, "g_fwd").wait_recv()
        copy(ch, "g_far").start()
        copy(ch, "p_bwd").start()
        copy(ch, "g_bwd").wait_recv()
        copy(ch, "p_fwd").start()
        yield "gather"
        copy(ch, "g_far").wait_recv()
        copy(ch, "p_far").start()
        yield "far"
        for name in ("p_own", "p_bwd", "p_fwd", "p_far"):
            copy(ch, name).wait_recv()
        for name in COPIES:
            copy(ch, name).wait_send()
        yield "end"

    order = (
        [f"x{p}" for p in range(NP)] + ["near"] + [f"z{p}" for p in range(NP)] + ["norm", "gather", "far", "end"]
    )

    def upto(steps_left, name):
        if steps_left is None or name is None:
            return
        gen, at = steps_left
        while at[0] <= order.index(name):
            assert next(gen) == order[at[0]]
            at[0] += 1

    n_col = 512

    def partial(ch, product, own):
        for p in range(NP):
            def body(n, _):
                cols = pl.ds(pl.multiple_of(n * n_col, n_col), n_col)
                pbuf[ch, :, :, :, cols] = product(cols).astype(BF).reshape(chips, 2, rows, n_col)
                return 0

            lax.fori_loop(p * piece // n_col, (p + 1) * piece // n_col, body, 0)
            copy(ch, f"part{p}").start()
            if p >= LAG:
                upto(own, f"x{p - LAG}")

    def normed(ch):
        return cbuf[ch].reshape(chunk, width)

    def attention(layer, ch, own):
        tok = pl.ds(ch * chunk, chunk)
        ct, st = cos[tok, :], sin[tok, :]

        def rope(v):
            return (v * ct + pltpu.roll(v, head // 2, 1) * st).astype(BF).astype(F32)

        for t in range(n_q):
            if ch == 0:
                finish(load_q(layer, t))
            q2 = dot(normed(ch), wa[t])
            for i in range(TILE // head):
                h = t * (TILE // head) + i
                qs[pl.ds(h, chunk, stride=heads), :] = rope(q2[:, i * head:(i + 1) * head])
        if ch == 0:
            finish(load_kv(layer))
        kv = dot(normed(ch), wa[n_q])
        k_new = rope(kv[:, :head])
        v_new = kv[:, head:].astype(BF).astype(F32)
        for h in range(heads):
            kx[pl.ds(h, chunk, stride=heads), :] = k_new
            vx[pl.ds(h, chunk, stride=heads), :] = v_new
        if ch == CHUNKS - 1:
            for t in range(n_attn):
                begin(load_a(layer, t))
        yield "qkv"

        def step(i, _):
            g = (layer * CHUNKS + ch) * steps + i
            slot = lax.rem(g, NKV)
            finish(load_cache(g))
            qrows = GRP * heads
            row_tok = lax.broadcasted_iota(jnp.int32, (qrows, head), 0) // heads
            pos = lax.broadcasted_iota(jnp.int32, (qrows, head), 1)
            for j in range(TOK // GRP):
                r = pl.ds(pl.multiple_of((i * (TOK // GRP) + j) * qrows, qrows), qrows)
                rn = pl.ds(pl.multiple_of(ch * chunk * heads + (i * (TOK // GRP) + j) * qrows, qrows), qrows)
                q = qs[r, :]
                kg = kbuf[slot, pl.ds(j * GRP, GRP)].reshape(GRP * kbuf.shape[2], head)
                vg = vbuf[slot, pl.ds(j * GRP, GRP)].reshape(GRP * kbuf.shape[2], head)
                lg = lax.dot_general(q.astype(BF), kg, (((1,), (1,)), ((), ())), preferred_element_type=F32) * scale
                n = nrow[rn, :]
                parts = [
                    jnp.where(pos < jnp.where(row_tok == b, n, 0), lg[:, b * head:(b + 1) * head], -1e30)
                    for b in range(GRP)
                ]
                l_new = jnp.sum(q * kx[r, :], axis=-1, keepdims=True) * scale
                top = functools.reduce(jnp.maximum, parts)
                m = jnp.maximum(jnp.max(top, axis=-1, keepdims=True), l_new)
                ps = [jnp.exp(b - m) for b in parts]
                p_new = jnp.exp(l_new - m)
                total = jnp.sum(functools.reduce(jnp.add, ps), axis=-1, keepdims=True) + p_new
                o = dot(jnp.concatenate(ps, axis=1).astype(BF), vg)
                o = o + p_new.astype(BF).astype(F32) * vx[r, :]
                osc[r, :] = o / total

            @pl.when(g + NKV < n_layers * CHUNKS * steps)
            def _():
                begin(load_cache(g + NKV), 0)

            return 0

        for lo, hi in ((0, steps // 2), (steps // 2, steps)):
            lax.fori_loop(lo, hi, step, 0)
            yield lo

        for h in range(heads):
            obf[:, h * head:(h + 1) * head] = osc[pl.ds(h, chunk, stride=heads), :].astype(BF)
        if ch == 0:
            for t in range(n_o):
                finish(load_o(layer, t))

        def product(cols):
            return functools.reduce(
                jnp.add, [dot(obf[:, t * TILE:(t + 1) * TILE], wb[t, :, cols]) for t in range(n_o)]
            )

        partial(ch, product, own)
        if ch == CHUNKS - 1:
            for t in range(n_o):
                begin(load_d(layer, t))

    def mlp(layer, ch, own):
        more = ch == CHUNKS - 1 and layer + 1 < n_layers

        def gate_up(j, _):
            if ch == 0:
                for t, src in enumerate((wg, wu)):
                    pltpu.make_async_copy(src.at[layer, :, pl.ds(0, TILE)], wa.at[2 * j + t], sem_a.at[2 * j + t]).wait()
            gate = dot(normed(ch), wa[2 * j])
            up = dot(normed(ch), wa[2 * j + 1])
            act[j] = (gate * (1.0 / (1.0 + jnp.exp(-gate))) * up).astype(BF)
            return 0

        for lo, hi in ((0, 3), (3, 5), (5, n_ff)):
            lax.fori_loop(lo, hi, gate_up, 0)
            if more:
                for t in range(2 * lo, 2 * hi):
                    if t < n_q:
                        begin(load_q(layer + 1, t))
                    elif t == n_q:
                        begin(load_kv(layer + 1))
                    else:
                        begin(load_a(layer + 1, t))
            yield lo
        if ch == 0:
            for t in range(n_ff):
                finish(load_d(layer, t))

        def product(cols):
            return functools.reduce(jnp.add, [dot(act[t], wb[t, :, cols]) for t in range(n_ff)])

        partial(ch, product, own)
        if more:
            for t in range(n_ff):
                begin(load_o(layer + 1, t) if t < n_o else load_d(layer + 1, t))

    stages = [(kind, layer, ch) for layer in range(n_layers) for kind in ("attn", "mlp") for ch in range(CHUNKS)]
    other = None
    for kind, layer, ch in stages:
        last = kind == "mlp" and layer + 1 == n_layers
        gain = mn.at[layer:layer + 1] if kind == "attn" else an.at[(layer + 1) % n_layers:(layer + 1) % n_layers + 1]
        own = (exchange(ch, gain, last), [0])
        if kind == "attn":
            if layer == 0:
                first_norm(ch)
            for done in attention(layer, ch, own):
                upto(other, {"qkv": f"z{NP - 1}", 0: None}.get(done, "norm"))
        else:
            for done in mlp(layer, ch, own):
                upto(other, {0: f"z{NP - 1}", 3: "norm"}.get(done, "norm"))
        for p in range(NP - LAG, NP):
            upto(own, f"x{p}")
        upto(own, "near")
        upto(other, "gather")
        upto(own, "z0")
        upto(other, "far")
        upto(own, "z1")
        upto(other, "end")
        other = own
    upto(other, "end")
    outs = [pltpu.make_async_copy(cbuf.at[ch], out.at[ch], sem_x.at[ch, 0]) for ch in range(CHUNKS)]
    begin(outs)
    finish(outs)


def solution(mesh):
    cache_spec = P(None, "dp", None, "tp", None)
    col_spec = P(None, None, "tp")
    row_spec = P(None, "tp", None)
    in_specs = (P("dp", None), P("dp"), cache_spec, cache_spec, P(), P(), col_spec, col_spec, col_spec, row_spec, col_spec, col_spec, row_spec)

    def local_layers(x, lengths, k_cache, v_cache, attn_norm, mlp_norm, w_q, w_k, w_v, w_o, w_gate, w_up, w_down):
        batch, width = x.shape
        layers, _, seq, _, head = k_cache.shape
        heads = w_q.shape[2] // head
        inner = w_o.shape[1]
        ff = w_gate.shape[2]
        n_tp = mesh.shape["tp"]
        chunk = batch // CHUNKS
        rows = chunk // n_tp
        split = (n_tp // 2, 2, rows, width)

        inv_freq = ROPE_BASE ** (-jnp.arange(0, head, 2).astype(F32) / head)
        angles = lengths.astype(F32)[:, None] * inv_freq[None, :]
        ct, st = jnp.cos(angles), jnp.sin(angles)
        cos = jnp.concatenate([ct, ct], axis=1)
        sin = jnp.concatenate([-st, st], axis=1)
        nrow = jnp.broadcast_to(lengths[:, None, None], (batch, heads, head)).reshape(batch * heads, head)

        vmem = pl.BlockSpec(memory_space=pltpu.VMEM)
        hbm = pl.BlockSpec(memory_space=pl.ANY)
        n_wa = 2 * (ff // TILE)
        n_wb = ff // TILE
        f32_rows = pltpu.VMEM((CHUNKS, rows, width), F32)
        y = pl.pallas_call(
            kernel,
            out_shape=jax.ShapeDtypeStruct((CHUNKS, *split), BF),
            in_specs=[hbm, vmem, vmem, vmem, hbm, hbm, vmem, vmem] + [hbm] * 7,
            out_specs=hbm,
            scratch_shapes=[
                pltpu.VMEM((n_wa, width, TILE), BF),
                pltpu.VMEM((n_wb, TILE, width), BF),
                pltpu.VMEM((NKV, TOK, seq, head), BF),
                pltpu.VMEM((NKV, TOK, seq, head), BF),
                pltpu.VMEM((CHUNKS, *split), BF),
                pltpu.VMEM((CHUNKS, *split), BF),
                pltpu.VMEM((CHUNKS, n_tp // 2, rows, width), BF),
                f32_rows, f32_rows, f32_rows, f32_rows, f32_rows, f32_rows,
                pltpu.VMEM((CHUNKS, rows, width), BF),
                pltpu.VMEM((n_wb, chunk, TILE), BF),
                pltpu.VMEM((chunk * heads, head), F32),
                pltpu.VMEM((chunk * heads, head), F32),
                pltpu.VMEM((chunk * heads, head), F32),
                pltpu.VMEM((chunk * heads, head), F32),
                pltpu.VMEM((chunk, inner), BF),
                pltpu.SemaphoreType.DMA((n_wa,)),
                pltpu.SemaphoreType.DMA((n_wb,)),
                pltpu.SemaphoreType.DMA((NKV + 1,)),
                pltpu.SemaphoreType.DMA((NKV,)),
                pltpu.SemaphoreType.DMA((CHUNKS, 2)),
                pltpu.SemaphoreType.DMA((CHUNKS, len(COPIES))),
                pltpu.SemaphoreType.DMA((CHUNKS, len(COPIES))),
            ],
            compiler_params=pltpu.CompilerParams(
                collective_id=0, has_side_effects=True, vmem_limit_bytes=67043328
            ),
            name="decoder",
        )(
            x.reshape(CHUNKS, *split), cos, sin, nrow,
            k_cache.reshape(layers, batch, seq, head), v_cache.reshape(layers, batch, seq, head),
            attn_norm, mlp_norm, w_q, w_k, w_v, w_o, w_gate, w_up, w_down,
        )
        return y.reshape(batch, width)

    return jax.shard_map(local_layers, mesh=mesh, in_specs=in_specs, out_specs=P("dp", None), check_vma=False)
```

```python
import functools

import jax
import jax.numpy as jnp
from jax import lax
from jax.experimental import pallas as pl
from jax.experimental.pallas import tpu as pltpu
from jax.sharding import PartitionSpec as P

NORM_EPS = 1e-5
ROPE_BASE = 10000.0
BF = jnp.bfloat16
F32 = jnp.float32
CHUNKS = 2
TOK = 16
NKV = 4
PAIR = 2
GRP = 4
TILE = 256
NP = 4
H_CUT = (0, 3, 4)
G_CUT = (0, 1, 6, 7)
PLAN = {'attn': {'q0': ('o:z2',),
          'q1': ('o:z3',),
          'h3': ('o:norm',),
          'h4': ('o:spread',),
          'p2': ('x0',),
          'p3': ('x1', 'o:gather'),
          'done': ('x2', 'x3', 'near', 'z0', 'o:far', 'z1', 'o:end')},
 'mlp': {'g1': ('o:z2', 'o:z3'),
         'g6': ('o:norm',),
         'g7': ('o:spread',),
         'p2': ('x0',),
         'p3': ('x1', 'o:gather'),
         'done': ('x2', 'x3', 'near', 'z0', 'o:far', 'z1', 'o:end')},
 'last': {'g1': ('o:z2', 'o:z3'),
          'g6': ('o:norm',),
          'g7': ('o:spread',),
          'p2': ('x0',),
          'p3': ('x1', 'o:gather'),
          'done': ('x2', 'x3', 'near', 'z0', 'z1', 'z2', 'o:far', 'z3', 'o:end')}}
ONCE = ("near", "g_fwd", "g_bwd", "g_far", "p_own", "p_bwd", "p_fwd", "p_far")
COPIES = ONCE + tuple(f"{k}{p}" for k in ("part", "far", "relay") for p in range(NP))


def dot(a, b):
    return jnp.dot(a, b, preferred_element_type=F32)


def kernel(
    x, lengths, freq, kc, vc, an, mn, wq, wk, wv, wo, wg, wu, wd, out,
    wa, wb, kbuf, vbuf, cbuf, pbuf, dbuf, xs, ys, zs, xr, yr, zr, hres, act, qs, kx, vx, osc, obf, cos, sin, nrow,
    sem_a, sem_b, sem_k, sem_v, sem_x, ssem, rsem,
):
    n_layers = wq.shape[0]
    width = x.shape[-1]
    n_tp = lax.axis_size("tp")
    chunk = n_tp * x.shape[3]
    head = kc.shape[3]
    heads = wq.shape[2] // head
    n_ff = wg.shape[2] // TILE
    n_o = wo.shape[1] // TILE
    n_q = wq.shape[2] // TILE
    chips = n_tp // 2
    rows = chunk // n_tp
    piece = width // NP
    steps = chunk // TOK
    scale = head ** -0.5

    me = lax.axis_index("tp")
    core = lax.rem(me, 2)
    chip = lax.div(me, 2)
    sign = 1 - 2 * core
    fwd_chip = lax.rem(chip + sign + chips, chips)
    bwd_chip = lax.rem(chip - sign + chips, chips)
    far_chip = lax.rem(chip + 2, chips)
    fwd, bwd = fwd_chip * 2 + core, bwd_chip * 2 + core
    peer = chip * 2 + 1 - core

    def load_a(layer, t):
        src = (wg, wu)[t % 2]
        return [pltpu.make_async_copy(src.at[layer, :, pl.ds((t // 2) * TILE, TILE)], wa.at[t], sem_a.at[t])]

    def load_q(layer, t):
        return [pltpu.make_async_copy(wq.at[layer, :, pl.ds(t * TILE, TILE)], wa.at[t], sem_a.at[t])]

    def load_kv(layer):
        t = n_q
        return [
            pltpu.make_async_copy(wk.at[layer], wa.at[t, :, pl.ds(0, head)], sem_a.at[t]),
            pltpu.make_async_copy(wv.at[layer], wa.at[t, :, pl.ds(head, head)], sem_k.at[NKV]),
        ]

    def load_o(layer, t):
        return [pltpu.make_async_copy(wo.at[layer, pl.ds(t * TILE, TILE), :], wb.at[t], sem_b.at[t])]

    def load_d(layer, t):
        return [pltpu.make_async_copy(wd.at[layer, pl.ds(t * TILE, TILE), :], wb.at[t], sem_b.at[t])]

    def begin(copies, priority=1):
        for c in copies:
            c.start(priority=priority)

    def finish(copies):
        for c in copies:
            c.wait()

    def load_cache(g):
        layer = g // (CHUNKS * steps)
        tok = pl.multiple_of(lax.rem(g, CHUNKS * steps) * TOK, TOK)
        slot = lax.rem(g, NKV)
        return [
            pltpu.make_async_copy(kc.at[layer, pl.ds(tok, TOK)], kbuf.at[slot], sem_k.at[slot]),
            pltpu.make_async_copy(vc.at[layer, pl.ds(tok, TOK)], vbuf.at[slot], sem_v.at[slot]),
        ]

    def load_x(ch):
        return [
            pltpu.make_async_copy(x.at[ch], pbuf.at[ch], sem_x.at[ch, 0]),
            pltpu.make_async_copy(x.at[ch, chip, core], hres.at[ch], sem_x.at[ch, 1]),
        ]

    n_attn = n_q + 1

    begin(load_x(0), 0)
    for t in range(n_q):
        begin(load_q(0, t), 0)
    begin(load_kv(0), 0)

    def load_rest():
        for g in range(NKV):
            begin(load_cache(jnp.int32(g)), 0)
        begin(load_x(1), 0)
        for t in range(n_o):
            begin(load_o(0, t))
        for t in range(n_attn, 2 * n_ff):
            begin(load_a(0, t))
        for t in range(n_o, n_ff):
            begin(load_d(0, t))

    barrier = pltpu.get_barrier_semaphore()
    for other in (peer, fwd, bwd):
        pl.semaphore_signal(barrier, inc=1, device_id={"tp": other}, device_id_type=pl.DeviceIdType.MESH)

    def tables(ch):
        n = jnp.broadcast_to(lengths[ch:ch + 1, :].astype(F32), (chunk, chunk)).T
        tok = pl.ds(ch * chunk, chunk)
        angles = n[:, :head] * freq[...]
        turn = jnp.sin(angles)
        cos[tok, :] = jnp.cos(angles)
        sin[tok, :] = jnp.where(lax.broadcasted_iota(jnp.int32, (chunk, head), 1) < head // 2, -turn, turn)
        for h in range(heads):
            nrow[pl.ds(ch * chunk * heads + h, chunk, stride=heads), :] = n[:, :head].astype(jnp.int32)

    def first_norm(ch):
        tables(ch)
        finish(load_x(ch))
        if ch == 0:
            load_rest()

        def body(i, _):
            c, k = i // 2, lax.rem(i, 2)
            h = pbuf[ch, c, k].astype(F32)
            inv = lax.rsqrt(jnp.mean(h * h, axis=-1, keepdims=True) + NORM_EPS)
            cbuf[ch, c, k] = (h * inv * an[0:1, :]).astype(BF)
            return 0

        lax.fori_loop(0, n_tp, body, 0)

    def cols_of(p):
        return pl.ds(p * piece, piece)

    def remote(ch, name, src, dst, target):
        i = COPIES.index(name)
        return pltpu.make_async_remote_copy(
            src_ref=src,
            dst_ref=dst,
            send_sem=ssem.at[ch, i],
            recv_sem=rsem.at[ch, i],
            device_id={"tp": target},
            device_id_type=pl.DeviceIdType.MESH,
        )

    def copy(ch, name):
        if name in ONCE:
            if name == "near":
                return remote(ch, name, ys.at[ch], yr.at[ch], bwd)
            c, target = {
                "g_fwd": (chip, fwd), "g_bwd": (chip, bwd), "g_far": (bwd_chip, fwd),
                "p_own": (chip, peer), "p_bwd": (bwd_chip, peer), "p_fwd": (fwd_chip, peer), "p_far": (far_chip, peer),
            }[name]
            return remote(ch, name, cbuf.at[ch, c, core], cbuf.at[ch, c, core], target)
        p = int(name[-1])
        if name.startswith("part"):
            return remote(ch, name, pbuf.at[ch, :, 1 - core, :, cols_of(p)], dbuf.at[ch, :, :, cols_of(p)], peer)
        if name.startswith("far"):
            return remote(ch, name, xs.at[ch, :, cols_of(p)], xr.at[ch, :, cols_of(p)], fwd)
        return remote(ch, name, zs.at[ch, :, cols_of(p)], zr.at[ch, :, cols_of(p)], fwd)

    def pair(ch, c, cols):
        return pbuf[ch, c, core, :, cols].astype(F32) + dbuf[ch, c, :, cols].astype(F32)

    def exchange(ch, gain, last):
        for p in range(NP):
            copy(ch, f"part{p}").wait_recv()
            xs[ch, :, cols_of(p)] = pair(ch, far_chip, cols_of(p))
            copy(ch, f"far{p}").start()
            yield f"x{p}"
        ys[ch] = pair(ch, bwd_chip, slice(None))
        copy(ch, "near").start()
        yield "near"
        for p in range(NP):
            copy(ch, f"far{p}").wait_recv()
            zs[ch, :, cols_of(p)] = xr[ch, :, cols_of(p)] + pair(ch, fwd_chip, cols_of(p))
            copy(ch, f"relay{p}").start()
            yield f"z{p}"
        copy(ch, "near").wait_recv()
        for p in range(NP):
            copy(ch, f"relay{p}").wait_recv()
        h = (hres[ch].astype(F32) + (pair(ch, chip, slice(None)) + yr[ch] + zr[ch])).astype(BF)
        if last:
            cbuf[ch, chip, core] = h
        else:
            hres[ch] = h
            hf = h.astype(F32)
            inv = lax.rsqrt(jnp.mean(hf * hf, axis=-1, keepdims=True) + NORM_EPS)
            cbuf[ch, chip, core] = (hf * inv * gain[...]).astype(BF)
        for name in ("g_fwd", "p_own"):
            copy(ch, name).start()
        yield "norm"
        copy(ch, "g_bwd").start()
        yield "spread"
        copy(ch, "g_fwd").wait_recv()
        copy(ch, "g_far").start()
        copy(ch, "p_bwd").start()
        yield "gather"
        copy(ch, "g_bwd").wait_recv()
        copy(ch, "p_fwd").start()
        yield "back"
        copy(ch, "g_far").wait_recv()
        copy(ch, "p_far").start()
        yield "far"
        for name in ("p_own", "p_bwd", "p_fwd", "p_far"):
            copy(ch, name).wait_recv()
        for name in COPIES:
            copy(ch, name).wait_send()
        yield "end"

    order = (
        [f"x{p}" for p in range(NP)] + ["near"] + [f"z{p}" for p in range(NP)] + ["norm", "spread", "gather", "back", "far", "end"]
    )

    def upto(steps_left, name):
        if steps_left is None or name is None:
            return
        gen, at = steps_left
        while at[0] <= order.index(name):
            with jax.named_scope(f"{order[at[0]]}"):
                assert next(gen) == order[at[0]]
            at[0] += 1

    n_col = 1024

    def partial(ch, product):
        for p in range(NP):
            def body(n, _):
                cols = pl.ds(pl.multiple_of(n * n_col, n_col), n_col)
                pbuf[ch, :, :, :, cols] = product(cols).astype(BF).reshape(chips, 2, rows, n_col)
                return 0

            with jax.named_scope("partial"):
                lax.fori_loop(p * piece // n_col, (p + 1) * piece // n_col, body, 0)
            copy(ch, f"part{p}").start()
            yield f"p{p}"

    def normed(ch):
        return cbuf[ch].reshape(chunk, width)

    def attention(layer, ch):
        tok = pl.ds(ch * chunk, chunk)
        ct, st = cos[tok, :], sin[tok, :]

        def rope(v):
            return (v * ct + pltpu.roll(v, head // 2, 1) * st).astype(BF).astype(F32)

        for t in range(n_q):
            if ch == 0:
                finish(load_q(layer, t))
            q2 = dot(normed(ch), wa[t])
            for i in range(TILE // head):
                h = t * (TILE // head) + i
                qs[pl.ds(h, chunk, stride=heads), :] = rope(q2[:, i * head:(i + 1) * head])
            yield f"q{t}"
        if ch == 0:
            finish(load_kv(layer))
        kv = dot(normed(ch), wa[n_q])
        k_new = rope(kv[:, :head])
        v_new = kv[:, head:].astype(BF).astype(F32)
        for h in range(heads):
            kx[pl.ds(h, chunk, stride=heads), :] = k_new
            vx[pl.ds(h, chunk, stride=heads), :] = v_new
        if ch == CHUNKS - 1:
            for t in range(n_attn):
                begin(load_a(layer, t))
        yield "qkv"

        seq = kbuf.shape[2]
        qrows = GRP * heads

        def step(i, _):
            first = (layer * CHUNKS + ch) * steps + i * PAIR
            for b in range(PAIR):
                finish(load_cache(first + b))
            row_tok = lax.broadcasted_iota(jnp.int32, (qrows, head), 0) // heads
            pos = lax.broadcasted_iota(jnp.int32, (qrows, head), 1)
            groups = [(b, j) for b in range(PAIR) for j in range(TOK // GRP)]

            def at(n, base=0):
                return pl.ds(pl.multiple_of(base + (i * len(groups) + n) * qrows, qrows), qrows)

            logits, probs = [], []
            for n, (b, j) in enumerate(groups):
                kg = kbuf[lax.rem(first + b, NKV), pl.ds(j * GRP, GRP)].reshape(GRP * seq, head)
                q = qs[at(n), :].astype(BF)
                logits.append(lax.dot_general(q, kg, (((1,), (1,)), ((), ())), preferred_element_type=F32) * scale)
            for n, lg in enumerate(logits):
                limit = nrow[at(n, ch * chunk * heads), :]
                parts = [
                    jnp.where(pos < jnp.where(row_tok == t, limit, 0), lg[:, t * seq:(t + 1) * seq], -1e30)
                    for t in range(GRP)
                ]
                l_new = jnp.sum(qs[at(n), :] * kx[at(n), :], axis=-1, keepdims=True) * scale
                m = jnp.maximum(jnp.max(functools.reduce(jnp.maximum, parts), axis=-1, keepdims=True), l_new)
                ps = [jnp.exp(t - m) for t in parts]
                p_new = jnp.exp(l_new - m)
                total = jnp.sum(functools.reduce(jnp.add, ps), axis=-1, keepdims=True) + p_new
                probs.append((jnp.concatenate(ps, axis=1).astype(BF), p_new, total))
            for n, (b, j) in enumerate(groups):
                p, p_new, total = probs[n]
                vg = vbuf[lax.rem(first + b, NKV), pl.ds(j * GRP, GRP)].reshape(GRP * seq, head)
                o = dot(p, vg) + p_new.astype(BF).astype(F32) * vx[at(n), :]
                osc[at(n), :] = o / total

            for b in range(PAIR):
                g = first + b

                @pl.when(g + NKV < n_layers * CHUNKS * steps)
                def _():
                    begin(load_cache(g + NKV), 0)

            return 0

        for lo, hi in zip(H_CUT, H_CUT[1:]):
            with jax.named_scope("heads"):
                lax.fori_loop(lo, hi, step, 0)
            yield f"h{hi}"

        if layer == 0 and ch == 0:
            pl.semaphore_wait(barrier, 3)
        for h in range(heads):
            obf[:, h * head:(h + 1) * head] = osc[pl.ds(h, chunk, stride=heads), :].astype(BF)
        if ch == 0:
            for t in range(n_o):
                finish(load_o(layer, t))

        def product(cols):
            return functools.reduce(
                jnp.add, [dot(obf[:, t * TILE:(t + 1) * TILE], wb[t, :, cols]) for t in range(n_o)]
            )

        yield from partial(ch, product)
        if ch == CHUNKS - 1:
            for t in range(n_o):
                begin(load_d(layer, t))

    def mlp(layer, ch):
        more = ch == CHUNKS - 1 and layer + 1 < n_layers

        def gate_up(j, _):
            if ch == 0:
                for t, src in enumerate((wg, wu)):
                    pltpu.make_async_copy(src.at[layer, :, pl.ds(0, TILE)], wa.at[2 * j + t], sem_a.at[2 * j + t]).wait()
            gate = dot(normed(ch), wa[2 * j])
            up = dot(normed(ch), wa[2 * j + 1])
            act[j] = (gate * (1.0 / (1.0 + jnp.exp(-gate))) * up).astype(BF)
            return 0

        for lo, hi in zip(G_CUT, G_CUT[1:]):
            with jax.named_scope("gateup"):
                lax.fori_loop(lo, hi, gate_up, 0)
            if more:
                for t in range(2 * lo, 2 * hi):
                    if t < n_q:
                        begin(load_q(layer + 1, t))
                    elif t == n_q:
                        begin(load_kv(layer + 1))
                    else:
                        begin(load_a(layer + 1, t))
            yield f"g{hi}"
        if ch == 0:
            for t in range(n_ff):
                finish(load_d(layer, t))

        def product(cols):
            return functools.reduce(jnp.add, [dot(act[t], wb[t, :, cols]) for t in range(n_ff)])

        yield from partial(ch, product)
        if more:
            for t in range(n_ff):
                begin(load_o(layer + 1, t) if t < n_o else load_d(layer + 1, t))

    stages = [(kind, layer, ch) for layer in range(n_layers) for kind in ("attn", "mlp") for ch in range(CHUNKS)]
    other = None
    for kind, layer, ch in stages:
        tags = attention(layer, ch) if kind == "attn" else mlp(layer, ch)
        last = kind == "mlp" and layer + 1 == n_layers
        gain = mn.at[layer:layer + 1] if kind == "attn" else an.at[(layer + 1) % n_layers:(layer + 1) % n_layers + 1]
        own = (exchange(ch, gain, last), [0])
        plan = PLAN["last" if last and ch == CHUNKS - 1 else kind]

        def run(tag):
            for step in plan.get(tag, ()):
                upto(other if step.startswith("o:") else own, step.removeprefix("o:"))

        if kind == "attn" and layer == 0:
            first_norm(ch)
        for tag in tags:
            run(tag)
        run("done")
        other = own
    upto(other, "end")
    outs = [pltpu.make_async_copy(cbuf.at[ch], out.at[ch], sem_x.at[ch, 0]) for ch in range(CHUNKS)]
    begin(outs)
    finish(outs)


def solution(mesh):
    cache_spec = P(None, "dp", None, "tp", None)
    col_spec = P(None, None, "tp")
    row_spec = P(None, "tp", None)
    in_specs = (P("dp", None), P("dp"), cache_spec, cache_spec, P(), P(), col_spec, col_spec, col_spec, row_spec, col_spec, col_spec, row_spec)

    def local_layers(x, lengths, k_cache, v_cache, attn_norm, mlp_norm, w_q, w_k, w_v, w_o, w_gate, w_up, w_down):
        batch, width = x.shape
        layers, _, seq, _, head = k_cache.shape
        heads = w_q.shape[2] // head
        inner = w_o.shape[1]
        ff = w_gate.shape[2]
        n_tp = mesh.shape["tp"]
        chunk = batch // CHUNKS
        rows = chunk // n_tp
        split = (n_tp // 2, 2, rows, width)

        freq = ROPE_BASE ** (-jnp.arange(0, head, 2).astype(F32) / head)
        freq = jnp.concatenate([freq, freq])[None, :]

        vmem = pl.BlockSpec(memory_space=pltpu.VMEM)
        hbm = pl.BlockSpec(memory_space=pl.ANY)
        n_wa = 2 * (ff // TILE)
        n_wb = ff // TILE
        f32_rows = pltpu.VMEM((CHUNKS, rows, width), F32)
        y = pl.pallas_call(
            kernel,
            out_shape=jax.ShapeDtypeStruct((CHUNKS, *split), BF),
            in_specs=[hbm, vmem, vmem, hbm, hbm, vmem, vmem] + [hbm] * 7,
            out_specs=hbm,
            scratch_shapes=[
                pltpu.VMEM((n_wa, width, TILE), BF),
                pltpu.VMEM((n_wb, TILE, width), BF),
                pltpu.VMEM((NKV, TOK, seq, head), BF),
                pltpu.VMEM((NKV, TOK, seq, head), BF),
                pltpu.VMEM((CHUNKS, *split), BF),
                pltpu.VMEM((CHUNKS, *split), BF),
                pltpu.VMEM((CHUNKS, n_tp // 2, rows, width), BF),
                f32_rows, f32_rows, f32_rows, f32_rows, f32_rows, f32_rows,
                pltpu.VMEM((CHUNKS, rows, width), BF),
                pltpu.VMEM((n_wb, chunk, TILE), BF),
                pltpu.VMEM((chunk * heads, head), F32),
                pltpu.VMEM((chunk * heads, head), F32),
                pltpu.VMEM((chunk * heads, head), F32),
                pltpu.VMEM((chunk * heads, head), F32),
                pltpu.VMEM((chunk, inner), BF),
                pltpu.VMEM((batch, head), F32),
                pltpu.VMEM((batch, head), F32),
                pltpu.VMEM((batch * heads, head), jnp.int32),
                pltpu.SemaphoreType.DMA((n_wa,)),
                pltpu.SemaphoreType.DMA((n_wb,)),
                pltpu.SemaphoreType.DMA((NKV + 1,)),
                pltpu.SemaphoreType.DMA((NKV,)),
                pltpu.SemaphoreType.DMA((CHUNKS, 2)),
                pltpu.SemaphoreType.DMA((CHUNKS, len(COPIES))),
                pltpu.SemaphoreType.DMA((CHUNKS, len(COPIES))),
            ],
            compiler_params=pltpu.CompilerParams(
                collective_id=0, has_side_effects=True, vmem_limit_bytes=67043328
            ),
            name="decoder",
        )(
            x.reshape(CHUNKS, *split), lengths.reshape(CHUNKS, chunk), freq,
            k_cache.reshape(layers, batch, seq, head), v_cache.reshape(layers, batch, seq, head),
            attn_norm, mlp_norm, w_q, w_k, w_v, w_o, w_gate, w_up, w_down,
        )
        return y.reshape(batch, width)

    return jax.shard_map(local_layers, mesh=mesh, in_specs=in_specs, out_specs=P("dp", None), check_vma=False)
```

```python
import functools

import jax
import jax.numpy as jnp
from jax import lax
from jax.experimental import pallas as pl
from jax.experimental.pallas import tpu as pltpu
from jax.sharding import PartitionSpec as P

NORM_EPS = 1e-5
ROPE_BASE = 10000.0
BF = jnp.bfloat16
F32 = jnp.float32
CHUNKS = 2
TOK = 16
NKV = 4
PAIR = 2
GRP = 4
TILE = 256
NP = 4
H_CUT = (0, 3, 4)
G_CUT = (0, 1, 6, 7)
PLAN = {'attn': {'q0': ('o:z2',),
          'q1': ('o:z3',),
          'h3': ('o:norm', 'o:spread'),
          'p2': ('x0',),
          'p3': ('x1', 'o:gather'),
          'done': ('x2', 'x3', 'near', 'z0', 'o:far', 'z1', 'o:end')},
 'mlp': {'g1': ('o:z2', 'o:z3'),
         'g6': ('o:norm', 'o:spread'),
         'p2': ('x0',),
         'p3': ('x1', 'o:gather'),
         'done': ('x2', 'x3', 'near', 'z0', 'o:far', 'z1', 'o:end')},
 'last': {'g1': ('o:z2', 'o:z3'),
          'g6': ('o:norm', 'o:spread'),
          'p2': ('x0',),
          'p3': ('x1', 'o:gather'),
          'done': ('x2', 'x3', 'near', 'z0', 'z1', 'z2', 'z3', 'o:far', 'o:end')}}
ONCE = ("near", "g_fwd", "g_bwd", "g_far", "p_own", "p_bwd", "p_fwd", "p_far")
COPIES = ONCE + tuple(f"{k}{p}" for k in ("part", "far", "relay") for p in range(NP))


def dot(a, b):
    return jnp.dot(a, b, preferred_element_type=F32)


def kernel(
    x, lengths, freq, kc, vc, an, mn, wq, wk, wv, wo, wg, wu, wd, out,
    wa, wb, kbuf, vbuf, cbuf, pbuf, dbuf, xs, ys, zs, xr, yr, zr, hres, act, qs, kx, vx, osc, obf, cos, sin, nrow,
    sem_a, sem_b, sem_k, sem_v, sem_x, ssem, rsem,
):
    n_layers = wq.shape[0]
    width = x.shape[-1]
    n_tp = lax.axis_size("tp")
    chunk = n_tp * x.shape[3]
    head = kc.shape[3]
    heads = wq.shape[2] // head
    n_ff = wg.shape[2] // TILE
    n_o = wo.shape[1] // TILE
    n_q = wq.shape[2] // TILE
    chips = n_tp // 2
    rows = chunk // n_tp
    piece = width // NP
    steps = chunk // TOK
    scale = head ** -0.5

    me = lax.axis_index("tp")
    core = lax.rem(me, 2)
    chip = lax.div(me, 2)
    sign = 1 - 2 * core
    fwd_chip = lax.rem(chip + sign + chips, chips)
    bwd_chip = lax.rem(chip - sign + chips, chips)
    far_chip = lax.rem(chip + 2, chips)
    fwd, bwd = fwd_chip * 2 + core, bwd_chip * 2 + core
    peer = chip * 2 + 1 - core

    def load_a(layer, t):
        src = (wg, wu)[t % 2]
        return [pltpu.make_async_copy(src.at[layer, :, pl.ds((t // 2) * TILE, TILE)], wa.at[t], sem_a.at[t])]

    def load_q(layer, t):
        return [pltpu.make_async_copy(wq.at[layer, :, pl.ds(t * TILE, TILE)], wa.at[t], sem_a.at[t])]

    def load_kv(layer):
        t = n_q
        return [
            pltpu.make_async_copy(wk.at[layer], wa.at[t, :, pl.ds(0, head)], sem_a.at[t]),
            pltpu.make_async_copy(wv.at[layer], wa.at[t, :, pl.ds(head, head)], sem_k.at[NKV]),
        ]

    def load_o(layer, t):
        return [pltpu.make_async_copy(wo.at[layer, pl.ds(t * TILE, TILE), :], wb.at[t], sem_b.at[t])]

    def load_d(layer, t):
        return [pltpu.make_async_copy(wd.at[layer, pl.ds(t * TILE, TILE), :], wb.at[t], sem_b.at[t])]

    def begin(copies, priority=1):
        for c in copies:
            c.start(priority=priority)

    def finish(copies):
        for c in copies:
            c.wait()

    def load_cache(g):
        layer = g // (CHUNKS * steps)
        tok = pl.multiple_of(lax.rem(g, CHUNKS * steps) * TOK, TOK)
        slot = lax.rem(g, NKV)
        return [
            pltpu.make_async_copy(kc.at[layer, pl.ds(tok, TOK)], kbuf.at[slot], sem_k.at[slot]),
            pltpu.make_async_copy(vc.at[layer, pl.ds(tok, TOK)], vbuf.at[slot], sem_v.at[slot]),
        ]

    def load_x(ch):
        return [
            pltpu.make_async_copy(x.at[ch], pbuf.at[ch], sem_x.at[ch, 0]),
            pltpu.make_async_copy(x.at[ch, chip, core], hres.at[ch], sem_x.at[ch, 1]),
        ]

    n_attn = n_q + 1

    begin(load_x(0), 0)
    for t in range(n_q):
        begin(load_q(0, t), 0)
    begin(load_kv(0), 0)

    def load_rest():
        for g in range(NKV):
            begin(load_cache(jnp.int32(g)), 0)
        begin(load_x(1), 0)
        for t in range(n_o):
            begin(load_o(0, t))
        for t in range(n_attn, 2 * n_ff):
            begin(load_a(0, t))
        for t in range(n_o, n_ff):
            begin(load_d(0, t))

    barrier = pltpu.get_barrier_semaphore()
    for other in (peer, fwd, bwd):
        pl.semaphore_signal(barrier, inc=1, device_id={"tp": other}, device_id_type=pl.DeviceIdType.MESH)

    def tables(ch):
        n = jnp.broadcast_to(lengths[ch:ch + 1, :].astype(F32), (chunk, chunk)).T
        tok = pl.ds(ch * chunk, chunk)
        angles = n[:, :head] * freq[...]
        turn = jnp.sin(angles)
        cos[tok, :] = jnp.cos(angles)
        sin[tok, :] = jnp.where(lax.broadcasted_iota(jnp.int32, (chunk, head), 1) < head // 2, -turn, turn)
        for h in range(heads):
            nrow[pl.ds(ch * chunk * heads + h, chunk, stride=heads), :] = n[:, :head].astype(jnp.int32)

    def first_norm(ch):
        tables(ch)
        finish(load_x(ch))
        if ch == 0:
            load_rest()

        def body(i, _):
            c, k = i // 2, lax.rem(i, 2)
            h = pbuf[ch, c, k].astype(F32)
            inv = lax.rsqrt(jnp.mean(h * h, axis=-1, keepdims=True) + NORM_EPS)
            cbuf[ch, c, k] = (h * inv * an[0:1, :]).astype(BF)
            return 0

        lax.fori_loop(0, n_tp, body, 0)

    def cols_of(p):
        return pl.ds(p * piece, piece)

    def remote(ch, name, src, dst, target):
        i = COPIES.index(name)
        return pltpu.make_async_remote_copy(
            src_ref=src,
            dst_ref=dst,
            send_sem=ssem.at[ch, i],
            recv_sem=rsem.at[ch, i],
            device_id={"tp": target},
            device_id_type=pl.DeviceIdType.MESH,
        )

    def copy(ch, name):
        if name in ONCE:
            if name == "near":
                return remote(ch, name, ys.at[ch], yr.at[ch], bwd)
            c, target = {
                "g_fwd": (chip, fwd), "g_bwd": (chip, bwd), "g_far": (bwd_chip, fwd),
                "p_own": (chip, peer), "p_bwd": (bwd_chip, peer), "p_fwd": (fwd_chip, peer), "p_far": (far_chip, peer),
            }[name]
            return remote(ch, name, cbuf.at[ch, c, core], cbuf.at[ch, c, core], target)
        p = int(name[-1])
        if name.startswith("part"):
            return remote(ch, name, pbuf.at[ch, :, 1 - core, :, cols_of(p)], dbuf.at[ch, :, :, cols_of(p)], peer)
        if name.startswith("far"):
            return remote(ch, name, xs.at[ch, :, cols_of(p)], xr.at[ch, :, cols_of(p)], fwd)
        return remote(ch, name, zs.at[ch, :, cols_of(p)], zr.at[ch, :, cols_of(p)], fwd)

    def pair(ch, c, cols):
        return pbuf[ch, c, core, :, cols].astype(F32) + dbuf[ch, c, :, cols].astype(F32)

    def exchange(ch, gain, last):
        for p in range(NP):
            copy(ch, f"part{p}").wait_recv()
            xs[ch, :, cols_of(p)] = pair(ch, far_chip, cols_of(p))
            copy(ch, f"far{p}").start()
            yield f"x{p}"
        ys[ch] = pair(ch, bwd_chip, slice(None))
        copy(ch, "near").start()
        yield "near"
        for p in range(NP):
            copy(ch, f"far{p}").wait_recv()
            zs[ch, :, cols_of(p)] = xr[ch, :, cols_of(p)] + pair(ch, fwd_chip, cols_of(p))
            copy(ch, f"relay{p}").start()
            yield f"z{p}"
        copy(ch, "near").wait_recv()
        for p in range(NP):
            copy(ch, f"relay{p}").wait_recv()
        h = (hres[ch].astype(F32) + (pair(ch, chip, slice(None)) + yr[ch] + zr[ch])).astype(BF)
        if last:
            cbuf[ch, chip, core] = h
        else:
            hres[ch] = h
            hf = h.astype(F32)
            inv = lax.rsqrt(jnp.mean(hf * hf, axis=-1, keepdims=True) + NORM_EPS)
            cbuf[ch, chip, core] = (hf * inv * gain[...]).astype(BF)
        for name in ("g_fwd", "p_own"):
            copy(ch, name).start()
        yield "norm"
        copy(ch, "g_bwd").start()
        yield "spread"
        copy(ch, "g_fwd").wait_recv()
        copy(ch, "g_far").start()
        copy(ch, "p_bwd").start()
        yield "gather"
        copy(ch, "g_bwd").wait_recv()
        copy(ch, "p_fwd").start()
        yield "back"
        copy(ch, "g_far").wait_recv()
        copy(ch, "p_far").start()
        yield "far"
        for name in ("p_own", "p_bwd", "p_fwd", "p_far"):
            copy(ch, name).wait_recv()
        for name in COPIES:
            copy(ch, name).wait_send()
        yield "end"

    order = (
        [f"x{p}" for p in range(NP)] + ["near"] + [f"z{p}" for p in range(NP)] + ["norm", "spread", "gather", "back", "far", "end"]
    )

    def upto(steps_left, name):
        if steps_left is None or name is None:
            return
        gen, at = steps_left
        while at[0] <= order.index(name):
            with jax.named_scope(f"{order[at[0]]}"):
                assert next(gen) == order[at[0]]
            at[0] += 1

    n_col = 1024

    def partial(ch, product):
        for p in range(NP):
            def body(n, _):
                cols = pl.ds(pl.multiple_of(n * n_col, n_col), n_col)
                pbuf[ch, :, :, :, cols] = product(cols).astype(BF).reshape(chips, 2, rows, n_col)
                return 0

            with jax.named_scope("partial"):
                lax.fori_loop(p * piece // n_col, (p + 1) * piece // n_col, body, 0)
            copy(ch, f"part{p}").start()
            yield f"p{p}"

    def normed(ch):
        return cbuf[ch].reshape(chunk, width)

    def attention(layer, ch):
        tok = pl.ds(ch * chunk, chunk)
        ct, st = cos[tok, :], sin[tok, :]

        def rope(v):
            return (v * ct + pltpu.roll(v, head // 2, 1) * st).astype(BF).astype(F32)

        for t in range(n_q):
            if ch == 0:
                finish(load_q(layer, t))
            q2 = dot(normed(ch), wa[t])
            for i in range(TILE // head):
                h = t * (TILE // head) + i
                qs[pl.ds(h, chunk, stride=heads), :] = rope(q2[:, i * head:(i + 1) * head])
            yield f"q{t}"
        if ch == 0:
            finish(load_kv(layer))
        kv = dot(normed(ch), wa[n_q])
        k_new = rope(kv[:, :head])
        v_new = kv[:, head:].astype(BF).astype(F32)
        for h in range(heads):
            kx[pl.ds(h, chunk, stride=heads), :] = k_new
            vx[pl.ds(h, chunk, stride=heads), :] = v_new
        if ch == CHUNKS - 1:
            for t in range(n_attn):
                begin(load_a(layer, t))
        yield "qkv"

        seq = kbuf.shape[2]
        qrows = GRP * heads

        def step(i, _):
            first = (layer * CHUNKS + ch) * steps + i * PAIR
            for b in range(PAIR):
                finish(load_cache(first + b))
            row_tok = lax.broadcasted_iota(jnp.int32, (qrows, head), 0) // heads
            pos = lax.broadcasted_iota(jnp.int32, (qrows, head), 1)
            groups = [(b, j) for b in range(PAIR) for j in range(TOK // GRP)]

            def at(n, base=0):
                return pl.ds(pl.multiple_of(base + (i * len(groups) + n) * qrows, qrows), qrows)

            logits, probs = [], []
            for n, (b, j) in enumerate(groups):
                kg = kbuf[lax.rem(first + b, NKV), pl.ds(j * GRP, GRP)].reshape(GRP * seq, head)
                q = qs[at(n), :].astype(BF)
                logits.append(lax.dot_general(q, kg, (((1,), (1,)), ((), ())), preferred_element_type=F32) * scale)
            for n, lg in enumerate(logits):
                limit = nrow[at(n, ch * chunk * heads), :]
                parts = [
                    jnp.where(pos < jnp.where(row_tok == t, limit, 0), lg[:, t * seq:(t + 1) * seq], -1e30)
                    for t in range(GRP)
                ]
                l_new = jnp.sum(qs[at(n), :] * kx[at(n), :], axis=-1, keepdims=True) * scale
                m = jnp.maximum(jnp.max(functools.reduce(jnp.maximum, parts), axis=-1, keepdims=True), l_new)
                ps = [jnp.exp(t - m) for t in parts]
                p_new = jnp.exp(l_new - m)
                total = jnp.sum(functools.reduce(jnp.add, ps), axis=-1, keepdims=True) + p_new
                probs.append((jnp.concatenate(ps, axis=1).astype(BF), p_new, total))
            for n, (b, j) in enumerate(groups):
                p, p_new, total = probs[n]
                vg = vbuf[lax.rem(first + b, NKV), pl.ds(j * GRP, GRP)].reshape(GRP * seq, head)
                o = dot(p, vg) + p_new.astype(BF).astype(F32) * vx[at(n), :]
                osc[at(n), :] = o / total

            for b in range(PAIR):
                g = first + b

                @pl.when(g + NKV < n_layers * CHUNKS * steps)
                def _():
                    begin(load_cache(g + NKV), 0)

            return 0

        for lo, hi in zip(H_CUT, H_CUT[1:]):
            with jax.named_scope("heads"):
                lax.fori_loop(lo, hi, step, 0)
            yield f"h{hi}"

        if layer == 0 and ch == 0:
            pl.semaphore_wait(barrier, 3)
        for h in range(heads):
            obf[:, h * head:(h + 1) * head] = osc[pl.ds(h, chunk, stride=heads), :].astype(BF)
        if ch == 0:
            for t in range(n_o):
                finish(load_o(layer, t))

        def product(cols):
            return functools.reduce(
                jnp.add, [dot(obf[:, t * TILE:(t + 1) * TILE], wb[t, :, cols]) for t in range(n_o)]
            )

        yield from partial(ch, product)
        if ch == CHUNKS - 1:
            for t in range(n_o):
                begin(load_d(layer, t))

    def mlp(layer, ch):
        more = ch == CHUNKS - 1 and layer + 1 < n_layers

        def gate_up(j, _):
            if ch == 0:
                for t, src in enumerate((wg, wu)):
                    pltpu.make_async_copy(src.at[layer, :, pl.ds(0, TILE)], wa.at[2 * j + t], sem_a.at[2 * j + t]).wait()
            gate = dot(normed(ch), wa[2 * j])
            up = dot(normed(ch), wa[2 * j + 1])
            act[j] = (gate * (1.0 / (1.0 + jnp.exp(-gate))) * up).astype(BF)
            return 0

        for lo, hi in zip(G_CUT, G_CUT[1:]):
            with jax.named_scope("gateup"):
                lax.fori_loop(lo, hi, gate_up, 0)
            if more:
                for t in range(2 * lo, 2 * hi):
                    if t < n_q:
                        begin(load_q(layer + 1, t))
                    elif t == n_q:
                        begin(load_kv(layer + 1))
                    else:
                        begin(load_a(layer + 1, t))
            yield f"g{hi}"
        if ch == 0:
            for t in range(n_ff):
                finish(load_d(layer, t))

        def product(cols):
            return functools.reduce(jnp.add, [dot(act[t], wb[t, :, cols]) for t in range(n_ff)])

        yield from partial(ch, product)
        if more:
            for t in range(n_ff):
                begin(load_o(layer + 1, t) if t < n_o else load_d(layer + 1, t))

    stages = [(kind, layer, ch) for layer in range(n_layers) for kind in ("attn", "mlp") for ch in range(CHUNKS)]
    other = None
    for kind, layer, ch in stages:
        tags = attention(layer, ch) if kind == "attn" else mlp(layer, ch)
        last = kind == "mlp" and layer + 1 == n_layers
        gain = mn.at[layer:layer + 1] if kind == "attn" else an.at[(layer + 1) % n_layers:(layer + 1) % n_layers + 1]
        own = (exchange(ch, gain, last), [0])
        plan = PLAN["last" if last and ch == CHUNKS - 1 else kind]

        def run(tag):
            for step in plan.get(tag, ()):
                upto(other if step.startswith("o:") else own, step.removeprefix("o:"))

        if kind == "attn" and layer == 0:
            first_norm(ch)
        for tag in tags:
            run(tag)
        run("done")
        other = own
    upto(other, "end")
    outs = [pltpu.make_async_copy(cbuf.at[ch], out.at[ch], sem_x.at[ch, 0]) for ch in range(CHUNKS)]
    begin(outs)
    finish(outs)


def solution(mesh):
    cache_spec = P(None, "dp", None, "tp", None)
    col_spec = P(None, None, "tp")
    row_spec = P(None, "tp", None)
    in_specs = (P("dp", None), P("dp"), cache_spec, cache_spec, P(), P(), col_spec, col_spec, col_spec, row_spec, col_spec, col_spec, row_spec)

    def local_layers(x, lengths, k_cache, v_cache, attn_norm, mlp_norm, w_q, w_k, w_v, w_o, w_gate, w_up, w_down):
        batch, width = x.shape
        layers, _, seq, _, head = k_cache.shape
        heads = w_q.shape[2] // head
        inner = w_o.shape[1]
        ff = w_gate.shape[2]
        n_tp = mesh.shape["tp"]
        chunk = batch // CHUNKS
        rows = chunk // n_tp
        split = (n_tp // 2, 2, rows, width)

        freq = ROPE_BASE ** (-jnp.arange(0, head, 2).astype(F32) / head)
        freq = jnp.concatenate([freq, freq])[None, :]

        vmem = pl.BlockSpec(memory_space=pltpu.VMEM)
        hbm = pl.BlockSpec(memory_space=pl.ANY)
        n_wa = 2 * (ff // TILE)
        n_wb = ff // TILE
        f32_rows = pltpu.VMEM((CHUNKS, rows, width), F32)
        y = pl.pallas_call(
            kernel,
            out_shape=jax.ShapeDtypeStruct((CHUNKS, *split), BF),
            in_specs=[hbm, vmem, vmem, hbm, hbm, vmem, vmem] + [hbm] * 7,
            out_specs=hbm,
            scratch_shapes=[
                pltpu.VMEM((n_wa, width, TILE), BF),
                pltpu.VMEM((n_wb, TILE, width), BF),
                pltpu.VMEM((NKV, TOK, seq, head), BF),
                pltpu.VMEM((NKV, TOK, seq, head), BF),
                pltpu.VMEM((CHUNKS, *split), BF),
                pltpu.VMEM((CHUNKS, *split), BF),
                pltpu.VMEM((CHUNKS, n_tp // 2, rows, width), BF),
                f32_rows, f32_rows, f32_rows, f32_rows, f32_rows, f32_rows,
                pltpu.VMEM((CHUNKS, rows, width), BF),
                pltpu.VMEM((n_wb, chunk, TILE), BF),
                pltpu.VMEM((chunk * heads, head), F32),
                pltpu.VMEM((chunk * heads, head), F32),
                pltpu.VMEM((chunk * heads, head), F32),
                pltpu.VMEM((chunk * heads, head), F32),
                pltpu.VMEM((chunk, inner), BF),
                pltpu.VMEM((batch, head), F32),
                pltpu.VMEM((batch, head), F32),
                pltpu.VMEM((batch * heads, head), jnp.int32),
                pltpu.SemaphoreType.DMA((n_wa,)),
                pltpu.SemaphoreType.DMA((n_wb,)),
                pltpu.SemaphoreType.DMA((NKV + 1,)),
                pltpu.SemaphoreType.DMA((NKV,)),
                pltpu.SemaphoreType.DMA((CHUNKS, 2)),
                pltpu.SemaphoreType.DMA((CHUNKS, len(COPIES))),
                pltpu.SemaphoreType.DMA((CHUNKS, len(COPIES))),
            ],
            compiler_params=pltpu.CompilerParams(
                collective_id=0, has_side_effects=True, vmem_limit_bytes=67043328
            ),
            name="decoder",
        )(
            x.reshape(CHUNKS, *split), lengths.reshape(CHUNKS, chunk), freq,
            k_cache.reshape(layers, batch, seq, head), v_cache.reshape(layers, batch, seq, head),
            attn_norm, mlp_norm, w_q, w_k, w_v, w_o, w_gate, w_up, w_down,
        )
        return y.reshape(batch, width)

    return jax.shard_map(local_layers, mesh=mesh, in_specs=in_specs, out_specs=P("dp", None), check_vma=False)
```
